32 devices in a mesh: gx: 2 (over core), gy: 4 (over y, x), gz: 4 (over z).
Axes of the slice: x: 2, y: 2, z: 4, core: 2. Of those that a mesh axis runs over, the one named last changes fastest.
Arguments:
- right_side: float32 [96, 192, 192], P('gx', 'gy', 'gz'), may hold values from -6 to 6
- face_coef: float32 [3, 96, 192, 192], P(None, 'gx', 'gy', 'gz'), may hold values from 0.3 to 3
- absorption: float32 [96, 192, 192], P('gx', 'gy', 'gz'), may hold values from 0.001 to 0.01
Outputs:
- solution: float32 [96, 192, 192], P('gx', 'gy', 'gz')
- residual: float32 [96, 192, 192], P('gx', 'gy', 'gz')
- relative_norm: float32 [], replicated
The draws below stay inside these ranges and needn't reach their ends.
All inputs are finite; a program needn't handle non-finite values.
Results may differ from the reference program's by a relative error of at most 0.0003.
Values sent between devices are 32-bit elements.
A program may use at most 192 MiB of HBM per device.

```python
import math
import jax
import jax.numpy as jnp
from jax import lax

LEVELS = 5
SWEEPS = 3
BOTTOM = 6
NX = 96
NY = 192
NZ = 192


def block_scale(stream_key, shape, cuts, low, top_value):
    def one(axis_at, blocks):
        draws = jax.random.uniform(jax.random.fold_in(jax.random.fold_in(stream_key, 6), axis_at), (blocks,), jnp.float32, low / len(cuts), top_value / len(cuts))
        return jnp.repeat(jnp.exp(draws), shape[axis_at] // blocks).reshape((-1,) + (1,) * (len(shape) - axis_at - 1))

    level = one(*cuts[0])
    for cut in cuts[1:]:
        level = level * one(*cut)
    return level


def noise(rng, shape, spread, bound, split=(), kind=jnp.bfloat16):
    entries = spread * jax.random.normal(rng, shape, jnp.float32)
    if split:
        entries = entries * block_scale(rng, shape, split, -0.22, 0.18)
    return jnp.clip(entries, -bound, bound).astype(kind)


def setup_inputs(seed: int = 0) -> dict:
    streams_of = jax.random.split(jax.random.key(seed), 4)
    return {
        "right_side": noise(streams_of[0], (NX, NY, NZ), 1.0, 6.0, ((0, 2), (1, 4), (2, 4)), jnp.float32),
        "face_coef": jnp.clip(jnp.exp(math.log(3.0) - 2.3025851 * jax.random.uniform(streams_of[1], (3, NX, NY, NZ), jnp.float32) ** block_scale(streams_of[1], (3, NX, NY, NZ), ((1, 2), (2, 4), (3, 4)), -0.2, 0.2)), 0.3, 3.0),
        "absorption": jnp.clip(jnp.exp(math.log(0.01) - 2.30258502 * jax.random.uniform(streams_of[2], (NX, NY, NZ), jnp.float32) ** block_scale(streams_of[2], (NX, NY, NZ), ((0, 2), (1, 4), (2, 4)), -0.2, 0.2)), 0.001, 0.01),
    }


cheb_low = 0.25
cheb_high = 2.0

def apply_stencil(field, stencil, weight, padded):
    low_x = padded[:-2, 1:-1, 1:-1]
    high_x = padded[2:, 1:-1, 1:-1]
    low_y = padded[1:-1, :-2, 1:-1]
    high_y = padded[1:-1, 2:, 1:-1]
    low_z = padded[1:-1, 1:-1, :-2]
    high_z = padded[1:-1, 1:-1, 2:]
    flux = stencil[0] * (field - low_x) + stencil[3] * (field - high_x)
    flux = flux + stencil[1] * (field - low_y) + stencil[4] * (field - high_y)
    flux = flux + stencil[2] * (field - low_z) + stencil[5] * (field - high_z)
    return stencil[6] * field + weight * flux

def inverse_diagonal(stencil, weight):
    total = stencil[0] + stencil[3] + stencil[1] + stencil[4] + stencil[2] + stencil[5]
    return 1.0 / (stencil[6] + weight * total)

def chebyshev(iterate, source, stencil, weight, sweeps, from_zero, pad_field):
    centre = 0.5 * (cheb_high + cheb_low)
    half_width = 0.5 * (cheb_high - cheb_low)
    cheb_ratio = centre / half_width
    cheb_rho = 1.0 / cheb_ratio
    scaling = inverse_diagonal(stencil, weight)
    if from_zero:
        remainder = source
    else:
        remainder = source - apply_stencil(iterate, stencil, weight, pad_field(iterate))
    update = scaling * remainder * (1.0 / centre)
    for sweep in range(sweeps):
        iterate = iterate + update
        if sweep + 1 < sweeps:
            remainder = source - apply_stencil(iterate, stencil, weight, pad_field(iterate))
            next_rho = 1.0 / (2.0 * cheb_ratio - cheb_rho)
            update = next_rho * cheb_rho * update + 2.0 * next_rho / half_width * (scaling * remainder)
            cheb_rho = next_rho
    return iterate

def conjugate(source, stencil, weight, pad_field, total):
    iterate = jnp.zeros_like(source)
    remainder = source
    search = source
    norm_now = total(remainder * remainder)
    for step in range(BOTTOM):
        applied = apply_stencil(search, stencil, weight, pad_field(search))
        step_size = norm_now / total(search * applied)
        iterate = iterate + step_size * search
        if step + 1 < BOTTOM:
            remainder = remainder - step_size * applied
            norm_next = total(remainder * remainder)
            search = remainder + norm_next / norm_now * search
            norm_now = norm_next
    return iterate

def average_cells(field):
    blocks = field.reshape(field.shape[0] // 2, 2, field.shape[1] // 2, 2, field.shape[2] // 2, 2)
    return lax.optimization_barrier(jnp.sum(blocks, axis=(1, 3, 5))) * 0.125

def average_faces(faces):
    halves = (faces.shape[1] // 2, 2, faces.shape[2] // 2, 2, faces.shape[3] // 2, 2)
    along_x = faces[0].reshape(halves)[:, 0]
    along_y = faces[1].reshape(halves)[:, :, :, 0]
    along_z = faces[2].reshape(halves)[..., 0]
    return jnp.stack([lax.optimization_barrier(jnp.sum(along_x, axis=(2, 4))), lax.optimization_barrier(jnp.sum(along_y, axis=(1, 4))), lax.optimization_barrier(jnp.sum(along_z, axis=(1, 3)))]) * 0.25

def repeat_cells(field):
    shape = field.shape
    wide = jnp.broadcast_to(field[:, None, :, None, :, None], (shape[0], 2, shape[1], 2, shape[2], 2))
    return wide.reshape(2 * shape[0], 2 * shape[1], 2 * shape[2])

def pad_zero(field):
    return jnp.pad(field, 1)

def build_stencil(faces, cells):
    high_x = jnp.pad(faces[0, 1:], ((0, 1), (0, 0), (0, 0)))
    high_y = jnp.pad(faces[1, :, 1:], ((0, 0), (0, 1), (0, 0)))
    high_z = jnp.pad(faces[2, :, :, 1:], ((0, 0), (0, 0), (0, 1)))
    return jnp.stack([faces[0], faces[1], faces[2], high_x, high_y, high_z, cells])

def reference(right_side, face_coef, absorption):
    stencils = []
    faces = face_coef
    cells = absorption
    for level in range(LEVELS):
        stencils.append(build_stencil(faces, cells))
        if level + 1 < LEVELS:
            faces = average_faces(faces)
            cells = average_cells(cells)
    sources = []
    iterates = []
    source = right_side
    for level in range(LEVELS - 1):
        weight = 0.25 ** level
        iterate = chebyshev(jnp.zeros_like(source), source, stencils[level], weight, SWEEPS, True, pad_zero)
        remainder = source - apply_stencil(iterate, stencils[level], weight, pad_zero(iterate))
        sources.append(source)
        iterates.append(iterate)
        source = average_cells(remainder)
    correction = conjugate(source, stencils[LEVELS - 1], 0.25 ** (LEVELS - 1), pad_zero, jnp.sum)
    for level in reversed(range(LEVELS - 1)):
        weight = 0.25 ** level
        iterate = iterates[level] + repeat_cells(correction)
        correction = chebyshev(iterate, sources[level], stencils[level], weight, SWEEPS, False, pad_zero)
    residual = right_side - apply_stencil(correction, stencils[0], 1.0, pad_zero(correction))
    relative_norm = jnp.sqrt(jnp.sum(residual * residual) / jnp.sum(right_side * right_side))
    return (correction, residual, relative_norm)
```

```python
import functools

import jax
import jax.numpy as jnp
from jax import lax
from jax.experimental import pallas as pl
from jax.experimental.pallas import tpu as pltpu
from jax.sharding import PartitionSpec as P

LEVELS = 5
SWEEPS = 3
BOTTOM = 6
LANES = 128
TOP = 8

cheb_low = 0.25
cheb_high = 2.0
AXES = ("gx", "gy", "gz")
PER_LEVEL = 11


def ceil8(n):
    return (n + 7) // 8 * 8


def chebyshev_factors():
    centre = 0.5 * (cheb_high + cheb_low)
    half_width = 0.5 * (cheb_high - cheb_low)
    ratio = centre / half_width
    rho = 1.0 / ratio
    factors = [(0.0, 1.0 / centre)]
    for _ in range(SWEEPS - 1):
        new = 1.0 / (2.0 * ratio - rho)
        factors.append((new * rho, 2.0 * new / half_width))
        rho = new
    return factors


def iota(shape, dim):
    return lax.broadcasted_iota(jnp.int32, shape, dim)


def lane_roll(value, shift):
    if isinstance(shift, int):
        shift = shift % LANES
        return value if shift == 0 else pltpu.roll(value, shift, 1)
    return pltpu.roll(value, lax.rem(shift + LANES, LANES), 1)


def product(a, b):
    return jnp.dot(
        a, b, precision=lax.Precision.HIGHEST, preferred_element_type=jnp.float32
    )


def kernel(sizes, counts, rhs_ref, face_ref, cell_ref, sol_ref, res_ref, norm_ref, *scratch):
    deepest = LEVELS - 1
    levels = []
    at = 0
    for level in range(LEVELS):
        levels.append(scratch[at : at + PER_LEVEL])
        at += PER_LEVEL
    (stage, ysend, zsend, recv, cysend, czsend, crecv,
     gsend, gz_recv, gy_send, gy_recv, gx_recv, glob, whole,
     nsend, nz_recv, ny_recv, nx_recv,
     send_sem, recv_sem, csend_sem, crecv_sem, gsend_sem, grecv_sem,
     nsend_sem, nrecv_sem) = scratch[at:]
    place = [lax.axis_index(a) for a in AXES]
    factors = chebyshev_factors()
    low_of = iota((LANES, LANES), 0)
    high_of = iota((LANES, LANES), 1)
    pair_sum = jnp.where(low_of // 2 == high_of, 1.0, 0.0)
    pick_even = jnp.where(low_of == 2 * high_of, 1.0, 0.0)
    spread = jnp.where(low_of == high_of // 2, 1.0, 0.0)

    for dim in range(3):
        @pl.when(place[dim] == 0)
        def _():
            for slot in range(2):
                recv[slot, 2 * dim] = jnp.zeros_like(recv[slot, 2 * dim])

        @pl.when(place[dim] == counts[dim] - 1)
        def _():
            for slot in range(2):
                recv[slot, 2 * dim + 1] = jnp.zeros_like(recv[slot, 2 * dim + 1])
            for level in range(deepest):
                crecv[level, dim] = jnp.zeros_like(crecv[level, dim])

    def loop(n, body, init=0, unroll=None):
        if unroll is None:
            unroll = 2 if n % 2 == 0 else 1
        return lax.fori_loop(0, n, body, init, unroll=unroll)

    def clear(ref):
        def one(i, c):
            ref[i] = jnp.zeros(ref.shape[1:], jnp.float32)
            return c
        loop(ref.shape[0], one, unroll=1)

    stage[...] = jnp.zeros_like(stage)
    for level in range(deepest):
        for ref in levels[level][:2]:
            clear(ref)
    n = sizes[0]
    for ref in levels[0][2:]:
        clear(ref)

    xa, xb, f, dd, diag, inv, bx, by, bz, hz, cells = levels[0]

    def load(i, acc):
        value = rhs_ref[i]
        f[i, :, 0:n] = value
        bx[i, :, 0:n] = face_ref[0, i]
        by[i, 0:n, 0:n] = face_ref[1, i]
        bz[i, :, 0:n] = face_ref[2, i]
        cells[i, :, 0:n] = cell_ref[i]
        return acc
    loop(n, load)

    def source_square(i, acc):
        value = levels[0][2][i]
        return acc + value * value
    rhs_square = loop(n, source_square, jnp.zeros((n, LANES), jnp.float32))

    def transfer(nc, pick, matrix, scale, store):
        rows = ceil8(nc)

        def first(i, c):
            stage[i, 0:nc, :] = pick(i)
            return c
        loop(nc, first)
        chunk = nc
        while chunk * rows > 160 and chunk % 2 == 0:
            chunk //= 2

        def second(i, c):
            block = stage[pl.ds(i * chunk, chunk), 0:rows, :].reshape(chunk * rows, LANES)
            out = (product(block, matrix) * scale).reshape(chunk, rows, LANES)
            store(i * chunk, chunk, rows, out)
            return c
        loop(nc // chunk, second, unroll=1)

    def to(ref):
        def store(start, chunk, rows, out):
            ref[pl.ds(start, chunk), 0:rows, :] = out
        return store

    for level in range(deepest):
        nc = sizes[level + 1]
        _, _, _, _, _, _, bx, by, bz, hz, cells = levels[level]
        _, _, _, _, _, _, bx_c, by_c, bz_c, _, cells_c = levels[level + 1]

        def rows(ref, i, odd):
            return ref[i, pl.ds(odd, nc, stride=2), :]

        def four(ref, i):
            return (rows(ref, 2 * i, 0) + rows(ref, 2 * i, 1)) + (
                rows(ref, 2 * i + 1, 0) + rows(ref, 2 * i + 1, 1)
            )
        transfer(nc, lambda i: rows(bx, 2 * i, 0) + rows(bx, 2 * i, 1), pair_sum, 0.0625, to(bx_c))
        transfer(nc, lambda i: rows(by, 2 * i, 0) + rows(by, 2 * i + 1, 0), pair_sum, 0.0625, to(by_c))
        transfer(nc, lambda i: four(bz, i), pick_even, 0.0625, to(bz_c))
        transfer(nc, lambda i: four(cells, i), pair_sum, 0.125, to(cells_c))

    def coef_copy(level, dim):
        n = sizes[level]
        wide = ceil8(n)
        bx = levels[level][6]
        src = (
            bx.at[0, pl.ds(0, wide)],
            cysend.at[level, pl.ds(0, wide)],
            czsend.at[level, pl.ds(0, wide)],
        )[dim]
        return pltpu.make_async_remote_copy(
            src_ref=src,
            dst_ref=crecv.at[level, dim, pl.ds(0, wide)],
            send_sem=csend_sem.at[level, dim],
            recv_sem=crecv_sem.at[level, dim],
            device_id={AXES[dim]: jnp.maximum(place[dim] - 1, 0)},
            device_id_type=pl.DeviceIdType.MESH,
        )

    for level in range(deepest):
        n = sizes[level]
        _, _, _, _, _, _, bx, by, bz, hz, cells = levels[level]
        lane = iota((n, LANES), 1)

        def faces(i, acc):
            cysend[level, pl.ds(i, 1), :] = by[i, 0:1, :]
            return jnp.where(lane == i, lane_roll(bz[i, 0:n, :], i), acc)
        czsend[level, 0:n, :] = loop(n, faces, jnp.zeros((n, LANES), jnp.float32))
        for dim in range(3):
            @pl.when(place[dim] > 0)
            def _():
                coef_copy(level, dim).start()
    for level in range(deepest):
        for dim in range(3):
            @pl.when(place[dim] > 0)
            def _():
                coef_copy(level, dim).wait_send()

            @pl.when(place[dim] < counts[dim] - 1)
            def _():
                coef_copy(level, dim).wait_recv()
        n = sizes[level]
        wide = ceil8(n)
        _, _, _, _, diag, inv, bx, by, bz, hz, cells = levels[level]
        lane = iota((n, LANES), 1)
        bx[n, 0:wide, :] = crecv[level, 0, 0:wide, :]

        def finish(i, c):
            by[i, n : n + 1, :] = crecv[level, 1, pl.ds(i, 1), :]
            here = bz[i, 0:n, :]
            edge = lane_roll(crecv[level, 2, 0:n, :], n - 1 - i)
            upper = jnp.where(lane == n - 1, edge, lane_roll(here, -1))
            upper = jnp.where(lane < n, upper, 0.0)
            hz[i, 0:n, :] = upper
            total = bx[i, 0:n, :] + bx[i + 1, 0:n, :] + by[i, 0:n, :] + by[i, 1 : n + 1, :]
            total = total + here + upper + cells[i, 0:n, :]
            total = jnp.where(lane < n, total, 1.0)
            diag[i, 0:n, :] = jnp.where(lane < n, total, 0.0)
            inv[i, 0:n, :] = jnp.where(lane < n, 1.0 / total, 0.0)
            return c
        loop(n, finish)

    tally = [0]

    def face_copy(level, field, slot, dim, up):
        n = sizes[level]
        wide = ceil8(n)
        toward = jnp.minimum(place[dim] + 1, counts[dim] - 1) if up else jnp.maximum(place[dim] - 1, 0)
        part = 1 if up else 0
        if dim == 0:
            src = field.at[n if up else 1, pl.ds(TOP, wide)]
        else:
            src = (ysend if dim == 1 else zsend).at[part, pl.ds(0, wide)]
        which = 2 * dim + (0 if up else 1)
        return pltpu.make_async_remote_copy(
            src_ref=src,
            dst_ref=recv.at[slot, which, pl.ds(0, wide)],
            send_sem=send_sem.at[slot, which],
            recv_sem=recv_sem.at[slot, which],
            device_id={AXES[dim]: toward},
            device_id_type=pl.DeviceIdType.MESH,
        )

    def sweep_planes(level, field, make):
        n = sizes[level]
        lane = iota((n, LANES), 1)

        def one(i, accs):
            value = make(i)
            field[i + 1, TOP : TOP + n, :] = value
            ysend[0, pl.ds(i, 1), :] = value[0:1]
            ysend[1, pl.ds(i, 1), :] = value[n - 1 : n]
            turned = lane_roll(value, i - (n - 1))
            low = jnp.where(lane == lax.rem(i - n + 1 + LANES, LANES), turned, accs[0])
            high = jnp.where(lane == i, turned, accs[1])
            return low, high
        zero = jnp.zeros((n, LANES), jnp.float32)
        low, high = loop(n, one, (zero, zero))
        zsend[0, 0:n, :] = low
        zsend[1, 0:n, :] = high

    def exchange(level, field):
        slot = tally[0] % 2
        tally[0] += 1
        n = sizes[level]
        wide = ceil8(n)
        for dim in (1, 2, 0):
            last = counts[dim] - 1

            @pl.when(place[dim] < last)
            def _():
                face_copy(level, field, slot, dim, True).start()

            @pl.when(place[dim] > 0)
            def _():
                face_copy(level, field, slot, dim, False).start()
        for dim in (0, 2, 1):
            last = counts[dim] - 1

            @pl.when(place[dim] < last)
            def _():
                face_copy(level, field, slot, dim, True).wait_send()
                face_copy(level, field, slot, dim, False).wait_recv()

            @pl.when(place[dim] > 0)
            def _():
                face_copy(level, field, slot, dim, False).wait_send()
                face_copy(level, field, slot, dim, True).wait_recv()
        field[0, TOP : TOP + wide, :] = recv[slot, 0, 0:wide, :]
        field[n + 1, TOP : TOP + wide, :] = recv[slot, 1, 0:wide, :]
        _, _, f, _, diag, _, bx, by, bz, hz, _ = levels[level]
        lane = iota((n, LANES), 1)
        row = iota((n, LANES), 0)

        def remainder(i):
            here = field[i + 1, TOP : TOP + n, :]
            low_y = jnp.where(
                row == 0, recv[slot, 2, pl.ds(i, 1), :], field[i + 1, TOP - 1 : TOP - 1 + n, :]
            )
            high_y = jnp.where(
                row == n - 1, recv[slot, 3, pl.ds(i, 1), :], field[i + 1, TOP + 1 : TOP + 1 + n, :]
            )
            low_z = jnp.where(
                lane == 0, lane_roll(recv[slot, 4, 0:n, :], LANES - i), lane_roll(here, 1)
            )
            high_z = jnp.where(
                lane == n - 1,
                lane_roll(recv[slot, 5, 0:n, :], 2 * n - 2 - i),
                lane_roll(here, -1),
            )
            out = f[i, 0:n, :] - diag[i, 0:n, :] * here
            out = out + bx[i, 0:n, :] * field[i, TOP : TOP + n, :]
            out = out + bx[i + 1, 0:n, :] * field[i + 2, TOP : TOP + n, :]
            flow = by[i, 0:n, :] * low_y + by[i, 1 : n + 1, :] * high_y
            flow = flow + bz[i, 0:n, :] * low_z + hz[i, 0:n, :] * high_z
            return out + flow
        return remainder

    def chebyshev_sweep(level, old, new, factor):
        keep, gain = factor
        remainder = exchange(level, old)
        n = sizes[level]
        dd, inv = levels[level][3], levels[level][5]

        def make(i):
            step = gain * (inv[i, 0:n, :] * remainder(i))
            if keep:
                step = step + keep * dd[i, 0:n, :]
            dd[i, 0:n, :] = step
            return old[i + 1, TOP : TOP + n, :] + step
        sweep_planes(level, new, make)

    for level in range(deepest):
        n, nc = sizes[level], sizes[level + 1]
        xa, xb, f, dd, diag, inv = levels[level][:6]

        def begin(i):
            step = factors[0][1] * (inv[i, 0:n, :] * f[i, 0:n, :])
            dd[i, 0:n, :] = step
            return step
        sweep_planes(level, xa, begin)
        chebyshev_sweep(level, xa, xb, factors[1])
        chebyshev_sweep(level, xb, xa, factors[2])
        remainder = exchange(level, xa)

        def pick(i):
            xb[1, TOP : TOP + n, :] = remainder(2 * i) + remainder(2 * i + 1)
            return xb[1, pl.ds(TOP, nc, stride=2), :] + xb[1, pl.ds(TOP + 1, nc, stride=2), :]
        transfer(nc, pick, pair_sum, 0.125, to(levels[level + 1][2]))

    m = sizes[deepest]
    f_b, bx_b, by_b, bz_b, cells_b = [levels[deepest][k] for k in (2, 6, 7, 8, 10)]
    gsend[...] = jnp.zeros_like(gsend)
    for which, ref in enumerate((f_b, bx_b, by_b, bz_b, cells_b)):
        for i in range(m):
            start = (which * m + i) * m
            gsend[start : start + m, :] = lane_roll(ref[i, 0:m, :], place[2] * m)

    def line(dim, src, dst, ssem, rsem):
        total = counts[dim]

        def copy(off):
            return pltpu.make_async_remote_copy(
                src_ref=src,
                dst_ref=dst.at[place[dim]],
                send_sem=ssem.at[dim, off],
                recv_sem=rsem.at[dim, off],
                device_id={AXES[dim]: lax.rem(place[dim] + off, total)},
                device_id_type=pl.DeviceIdType.MESH,
            )
        for off in range(1, total):
            copy(off).start()
        dst[place[dim]] = src[...]
        for off in range(1, total):
            copy(off).wait()

    line(2, gsend, gz_recv, gsend_sem, grecv_sem)
    merged = gz_recv[0]
    for k in range(1, counts[2]):
        merged = merged + gz_recv[k]
    gy_send[...] = merged
    line(1, gy_send, gy_recv, gsend_sem, grecv_sem)
    line(0, gy_recv, gx_recv, gsend_sem, grecv_sem)

    tall = glob.shape[2]
    mx, my, mz = m * counts[0], m * counts[1], m * counts[2]
    glob[...] = jnp.zeros_like(glob)
    for which in range(5):
        for a in range(counts[0]):
            for b in range(counts[1]):
                for i in range(m):
                    start = (which * m + i) * m
                    glob[which, a * m + i, b * m : (b + 1) * m, :] = gx_recv[
                        a, b, start : start + m, :
                    ]
    lane = iota((tall, LANES), 1)
    row = iota((tall, LANES), 0)
    zero = jnp.zeros((tall, LANES), jnp.float32)
    for i in range(mx):
        hy = jnp.where(row < my - 1, pltpu.roll(glob[2, i], tall - 1, 0), 0.0)
        hz = jnp.where(lane < mz - 1, pltpu.roll(glob[3, i], LANES - 1, 1), 0.0)
        hx = glob[1, i + 1] if i + 1 < mx else zero
        glob[5, i] = hy
        glob[6, i] = hz
        glob[7, i] = glob[4, i] + glob[1, i] + hx + glob[2, i] + hy + glob[3, i] + hz

    def total(parts):
        acc = parts[0]
        for part in parts[1:]:
            acc = acc + part
        return jnp.sum(jnp.sum(acc, axis=0, keepdims=True), axis=1, keepdims=True)

    rest = [glob[0, i] for i in range(mx)]
    search = rest
    iterate = [zero] * mx
    norm_now = total([v * v for v in rest])
    for step in range(BOTTOM):
        applied = []
        for i in range(mx):
            v = search[i]
            out = glob[7, i] * v
            if i:
                out = out - glob[1, i] * search[i - 1]
            if i + 1 < mx:
                out = out - glob[1, i + 1] * search[i + 1]
            out = out - glob[2, i] * pltpu.roll(v, 1, 0) - glob[5, i] * pltpu.roll(v, tall - 1, 0)
            out = out - glob[3, i] * pltpu.roll(v, 1, 1) - glob[6, i] * pltpu.roll(v, LANES - 1, 1)
            applied.append(out)
        size = norm_now / total([a * b for a, b in zip(search, applied)])
        iterate = [e + size * v for e, v in zip(iterate, search)]
        if step + 1 < BOTTOM:
            rest = [r - size * q for r, q in zip(rest, applied)]
            norm_next = total([v * v for v in rest])
            ratio = norm_next / norm_now
            search = [r + ratio * v for r, v in zip(rest, search)]
            norm_now = norm_next
    for i in range(mx):
        whole[i] = iterate[i]
    below = levels[deepest][3]
    lane = iota((m, LANES), 1)
    for i in range(m):
        plane = whole[place[0] * m + i]
        plane = pltpu.roll(plane, lax.rem(tall - place[1] * m + tall, tall), 0)
        plane = pltpu.roll(plane, lax.rem(LANES - place[2] * m + LANES, LANES), 1)
        below[i, 0:m, :] = jnp.where(lane < m, plane[0:m], 0.0)

    coarse = lambda i: below[i, 0:m, :]
    for level in reversed(range(deepest)):
        n, nc = sizes[level], sizes[level + 1]
        xa, xb = levels[level][:2]

        def add(start, chunk, rows, out):
            for k in range(chunk):
                for odd_x in range(2):
                    plane = 2 * (start + k) + odd_x + 1
                    for odd_y in range(2):
                        at_rows = pl.ds(TOP + odd_y, nc, stride=2)
                        xa[plane, at_rows, :] = xa[plane, at_rows, :] + out[k, 0:nc]
        transfer(nc, coarse, spread, 1.0, add)
        sweep_planes(level, xa, lambda i: xa[i + 1, TOP : TOP + n, :])
        chebyshev_sweep(level, xa, xb, factors[0])
        chebyshev_sweep(level, xb, xa, factors[1])
        chebyshev_sweep(level, xa, xb, factors[2])
        coarse = functools.partial(lambda ref, count, i: ref[i + 1, TOP : TOP + count, :], xb, n)

    n = sizes[0]
    xa, xb = levels[0][:2]
    remainder = exchange(0, xb)

    def finish(i, acc):
        out = remainder(i)
        sol_ref[i] = xb[i + 1, TOP : TOP + n, 0:n]
        res_ref[i] = out[:, 0:n]
        return acc + out * out
    res_square = loop(n, finish, jnp.zeros((n, LANES), jnp.float32))
    nsend[0, 0:1, :] = jnp.sum(res_square, axis=0, keepdims=True)
    nsend[0, 1:2, :] = jnp.sum(rhs_square, axis=0, keepdims=True)
    nsend[0, 2:8, :] = jnp.zeros((6, LANES), jnp.float32)
    for step, (dim, got) in enumerate(((2, nz_recv), (1, ny_recv), (0, nx_recv))):
        line(dim, nsend.at[step], got, nsend_sem, nrecv_sem)
        acc = got[0]
        for k in range(1, counts[dim]):
            acc = acc + got[k]
        if step < 2:
            nsend[step + 1] = acc
    sums = jnp.sum(acc, axis=1, keepdims=True)
    norm_ref[...] = jnp.broadcast_to(jnp.sqrt(sums[0:1] / sums[1:2]), norm_ref.shape)


def body(counts, right_side, face_coef, absorption):
    n = right_side.shape[0]
    sizes = [n >> level for level in range(LEVELS)]
    f32 = jnp.float32
    scratch = []
    for size in sizes:
        wide = ceil8(size)
        flat = pltpu.VMEM((size, wide, LANES), f32)
        field = pltpu.VMEM((size + 2, wide + 2 * TOP, LANES), f32)
        scratch += [field, field, flat, flat, flat, flat]
        scratch += [
            pltpu.VMEM((size + 1, wide, LANES), f32),
            pltpu.VMEM((size, wide + 8, LANES), f32),
            flat, flat, flat,
        ]
    wide = ceil8(n)
    half = ceil8(n // 2)
    m = sizes[-1]
    packed = ceil8(5 * m * m)
    tall = (m * counts[1] + 8) // 8 * 8
    most = max(counts)
    scratch += [
        pltpu.VMEM((n // 2, half, LANES), f32),
        pltpu.VMEM((2, wide, LANES), f32),
        pltpu.VMEM((2, wide, LANES), f32),
        pltpu.VMEM((2, 6, wide, LANES), f32),
        pltpu.VMEM((LEVELS - 1, wide, LANES), f32),
        pltpu.VMEM((LEVELS - 1, wide, LANES), f32),
        pltpu.VMEM((LEVELS - 1, 3, wide, LANES), f32),
        pltpu.VMEM((packed, LANES), f32),
        pltpu.VMEM((counts[2], packed, LANES), f32),
        pltpu.VMEM((packed, LANES), f32),
        pltpu.VMEM((counts[1], packed, LANES), f32),
        pltpu.VMEM((counts[0], counts[1], packed, LANES), f32),
        pltpu.VMEM((8, m * counts[0], tall, LANES), f32),
        pltpu.VMEM((m * counts[0], tall, LANES), f32),
        pltpu.VMEM((3, 8, LANES), f32),
        pltpu.VMEM((counts[2], 8, LANES), f32),
        pltpu.VMEM((counts[1], 8, LANES), f32),
        pltpu.VMEM((counts[0], 8, LANES), f32),
        pltpu.SemaphoreType.DMA((2, 6)),
        pltpu.SemaphoreType.DMA((2, 6)),
        pltpu.SemaphoreType.DMA((LEVELS - 1, 3)),
        pltpu.SemaphoreType.DMA((LEVELS - 1, 3)),
        pltpu.SemaphoreType.DMA((3, most)),
        pltpu.SemaphoreType.DMA((3, most)),
        pltpu.SemaphoreType.DMA((3, most)),
        pltpu.SemaphoreType.DMA((3, most)),
    ]
    vmem = pl.BlockSpec(memory_space=pltpu.VMEM)
    answer, residual, norm = pl.pallas_call(
        functools.partial(kernel, sizes, counts),
        out_shape=(
            jax.ShapeDtypeStruct(right_side.shape, f32),
            jax.ShapeDtypeStruct(right_side.shape, f32),
            jax.ShapeDtypeStruct((8, LANES), f32),
        ),
        in_specs=[vmem] * 3,
        out_specs=(vmem,) * 3,
        scratch_shapes=scratch,
        compiler_params=pltpu.CompilerParams(
            has_side_effects=True, vmem_limit_bytes=60 * 1024 * 1024
        ),
        name="vcycle",
    )(right_side, face_coef, absorption)
    return answer, residual, norm[0, 0]


def solution(mesh):
    counts = tuple(mesh.shape[a] for a in AXES)
    return jax.shard_map(
        functools.partial(body, counts),
        mesh=mesh,
        in_specs=(P("gx", "gy", "gz"), P(None, "gx", "gy", "gz"), P("gx", "gy", "gz")),
        out_specs=(P("gx", "gy", "gz"), P("gx", "gy", "gz"), P()),
        check_vma=False,
    )
```

```python
import functools

import jax
import jax.numpy as jnp
from jax import lax
from jax.experimental import pallas as pl
from jax.experimental.pallas import tpu as pltpu
from jax.sharding import PartitionSpec as P

LEVELS = 5
SWEEPS = 3
BOTTOM = 6
LANES = 128
TOP = 8

cheb_low = 0.25
cheb_high = 2.0
AXES = ("gx", "gy", "gz")
PER_LEVEL = 11


def ceil8(n):
    return (n + 7) // 8 * 8


def chebyshev_factors():
    centre = 0.5 * (cheb_high + cheb_low)
    half_width = 0.5 * (cheb_high - cheb_low)
    ratio = centre / half_width
    rho = 1.0 / ratio
    factors = [(0.0, 1.0 / centre)]
    for _ in range(SWEEPS - 1):
        new = 1.0 / (2.0 * ratio - rho)
        factors.append((new * rho, 2.0 * new / half_width))
        rho = new
    return factors


def iota(shape, dim):
    return lax.broadcasted_iota(jnp.int32, shape, dim)


def lane_roll(value, shift):
    if isinstance(shift, int):
        shift = shift % LANES
        return value if shift == 0 else pltpu.roll(value, shift, 1)
    return pltpu.roll(value, lax.rem(shift + LANES, LANES), 1)


def product(a, b):
    return jnp.dot(
        a, b, precision=lax.Precision.HIGHEST, preferred_element_type=jnp.float32
    )


def kernel(sizes, counts, rhs_ref, face_ref, cell_ref, sol_ref, res_ref, norm_ref, *scratch):
    deepest = LEVELS - 1
    levels = []
    at = 0
    for level in range(LEVELS):
        levels.append(scratch[at : at + PER_LEVEL])
        at += PER_LEVEL
    (stage, ysend, zsend, recv, cysend, czsend, crecv,
     gsend, gz_recv, gy_send, gy_recv, gx_recv, glob, whole,
     nsend, nz_recv, ny_recv, nx_recv,
     send_sem, recv_sem, csend_sem, crecv_sem, gsend_sem, grecv_sem,
     nsend_sem, nrecv_sem) = scratch[at:]
    place = [lax.axis_index(a) for a in AXES]
    factors = chebyshev_factors()
    low_of = iota((LANES, LANES), 0)
    high_of = iota((LANES, LANES), 1)
    pair_sum = jnp.where(low_of // 2 == high_of, 1.0, 0.0)
    pick_even = jnp.where(low_of == 2 * high_of, 1.0, 0.0)
    spread = jnp.where(low_of == high_of // 2, 1.0, 0.0)

    for dim in range(3):
        @pl.when(place[dim] == 0)
        def _():
            for slot in range(2):
                recv[slot, 2 * dim] = jnp.zeros_like(recv[slot, 2 * dim])

        @pl.when(place[dim] == counts[dim] - 1)
        def _():
            for slot in range(2):
                recv[slot, 2 * dim + 1] = jnp.zeros_like(recv[slot, 2 * dim + 1])
            for level in range(deepest):
                crecv[level, dim] = jnp.zeros_like(crecv[level, dim])

    def loop(n, body, init=0, unroll=None):
        if unroll is None:
            unroll = next(u for u in (4, 3, 2, 1) if n % u == 0)
        return lax.fori_loop(0, n, body, init, unroll=unroll)

    def clear(ref):
        def one(i, c):
            ref[i] = jnp.zeros(ref.shape[1:], jnp.float32)
            return c
        loop(ref.shape[0], one, unroll=1)

    stage[...] = jnp.zeros_like(stage)
    for level in range(deepest):
        for ref in levels[level][:2]:
            clear(ref)
    n = sizes[0]
    for ref in levels[0][2:]:
        clear(ref)

    xa, xb, f, dd, diag, inv, bx, by, bz, hz, cells = levels[0]

    def load(i, acc):
        value = rhs_ref[i]
        f[i, :, 0:n] = value
        bx[i, :, 0:n] = face_ref[0, i]
        by[i, 0:n, 0:n] = face_ref[1, i]
        bz[i, :, 0:n] = face_ref[2, i]
        cells[i, :, 0:n] = cell_ref[i]
        return acc
    loop(n, load)

    def source_square(i, acc):
        value = levels[0][2][i]
        return acc + value * value
    rhs_square = loop(n, source_square, jnp.zeros((n, LANES), jnp.float32))

    def transfer(nc, pick, matrix, scale, store):
        rows = ceil8(nc)

        def first(i, c):
            stage[i, 0:nc, :] = pick(i)
            return c
        loop(nc, first)
        chunk = nc
        while chunk * rows > 160 and chunk % 2 == 0:
            chunk //= 2

        def second(i, c):
            block = stage[pl.ds(i * chunk, chunk), 0:rows, :].reshape(chunk * rows, LANES)
            out = (product(block, matrix) * scale).reshape(chunk, rows, LANES)
            store(i * chunk, chunk, rows, out)
            return c
        loop(nc // chunk, second, unroll=1)

    def to(ref):
        def store(start, chunk, rows, out):
            ref[pl.ds(start, chunk), 0:rows, :] = out
        return store

    for level in range(deepest):
        nc = sizes[level + 1]
        _, _, _, _, _, _, bx, by, bz, hz, cells = levels[level]
        _, _, _, _, _, _, bx_c, by_c, bz_c, _, cells_c = levels[level + 1]

        def rows(ref, i, odd):
            return ref[i, pl.ds(odd, nc, stride=2), :]

        def four(ref, i):
            return (rows(ref, 2 * i, 0) + rows(ref, 2 * i, 1)) + (
                rows(ref, 2 * i + 1, 0) + rows(ref, 2 * i + 1, 1)
            )
        transfer(nc, lambda i: rows(bx, 2 * i, 0) + rows(bx, 2 * i, 1), pair_sum, 0.0625, to(bx_c))
        transfer(nc, lambda i: rows(by, 2 * i, 0) + rows(by, 2 * i + 1, 0), pair_sum, 0.0625, to(by_c))
        transfer(nc, lambda i: four(bz, i), pick_even, 0.0625, to(bz_c))
        transfer(nc, lambda i: four(cells, i), pair_sum, 0.125, to(cells_c))

    def coef_copy(level, dim):
        n = sizes[level]
        wide = ceil8(n)
        bx = levels[level][6]
        src = (
            bx.at[0, pl.ds(0, wide)],
            cysend.at[level, pl.ds(0, wide)],
            czsend.at[level, pl.ds(0, wide)],
        )[dim]
        return pltpu.make_async_remote_copy(
            src_ref=src,
            dst_ref=crecv.at[level, dim, pl.ds(0, wide)],
            send_sem=csend_sem.at[level, dim],
            recv_sem=crecv_sem.at[level, dim],
            device_id={AXES[dim]: jnp.maximum(place[dim] - 1, 0)},
            device_id_type=pl.DeviceIdType.MESH,
        )

    for level in range(deepest):
        n = sizes[level]
        _, _, _, _, _, _, bx, by, bz, hz, cells = levels[level]
        lane = iota((n, LANES), 1)

        def faces(i, acc):
            cysend[level, pl.ds(i, 1), :] = by[i, 0:1, :]
            return jnp.where(lane == i, lane_roll(bz[i, 0:n, :], i), acc)
        czsend[level, 0:n, :] = loop(n, faces, jnp.zeros((n, LANES), jnp.float32))
        for dim in range(3):
            @pl.when(place[dim] > 0)
            def _():
                coef_copy(level, dim).start()
    for level in range(deepest):
        for dim in range(3):
            @pl.when(place[dim] > 0)
            def _():
                coef_copy(level, dim).wait_send()

            @pl.when(place[dim] < counts[dim] - 1)
            def _():
                coef_copy(level, dim).wait_recv()
        n = sizes[level]
        wide = ceil8(n)
        _, _, _, _, diag, inv, bx, by, bz, hz, cells = levels[level]
        lane = iota((n, LANES), 1)
        bx[n, 0:wide, :] = crecv[level, 0, 0:wide, :]

        def finish(i, c):
            by[i, n : n + 1, :] = crecv[level, 1, pl.ds(i, 1), :]
            here = bz[i, 0:n, :]
            edge = lane_roll(crecv[level, 2, 0:n, :], n - 1 - i)
            upper = jnp.where(lane == n - 1, edge, lane_roll(here, -1))
            upper = jnp.where(lane < n, upper, 0.0)
            hz[i, 0:n, :] = upper
            total = bx[i, 0:n, :] + bx[i + 1, 0:n, :] + by[i, 0:n, :] + by[i, 1 : n + 1, :]
            total = total + here + upper + cells[i, 0:n, :]
            total = jnp.where(lane < n, total, 1.0)
            diag[i, 0:n, :] = jnp.where(lane < n, total, 0.0)
            inv[i, 0:n, :] = jnp.where(lane < n, 1.0 / total, 0.0)
            return c
        loop(n, finish)

    tally = [0]

    def face_copy(level, field, slot, dim, up):
        n = sizes[level]
        wide = ceil8(n)
        toward = jnp.minimum(place[dim] + 1, counts[dim] - 1) if up else jnp.maximum(place[dim] - 1, 0)
        part = 1 if up else 0
        if dim == 0:
            src = field.at[n if up else 1, pl.ds(TOP, wide)]
        else:
            src = (ysend if dim == 1 else zsend).at[part, pl.ds(0, wide)]
        which = 2 * dim + (0 if up else 1)
        return pltpu.make_async_remote_copy(
            src_ref=src,
            dst_ref=recv.at[slot, which, pl.ds(0, wide)],
            send_sem=send_sem.at[slot, which],
            recv_sem=recv_sem.at[slot, which],
            device_id={AXES[dim]: toward},
            device_id_type=pl.DeviceIdType.MESH,
        )

    def sweep_planes(level, field, make):
        n = sizes[level]
        lane = iota((n, LANES), 1)

        def one(i, accs):
            value = make(i)
            field[i + 1, TOP : TOP + n, :] = value
            ysend[0, pl.ds(i, 1), :] = value[0:1]
            ysend[1, pl.ds(i, 1), :] = value[n - 1 : n]
            turned = lane_roll(value, i - (n - 1))
            low = jnp.where(lane == lax.rem(i - n + 1 + LANES, LANES), turned, accs[0])
            high = jnp.where(lane == i, turned, accs[1])
            return low, high
        zero = jnp.zeros((n, LANES), jnp.float32)
        low, high = loop(n, one, (zero, zero))
        zsend[0, 0:n, :] = low
        zsend[1, 0:n, :] = high

    def exchange(level, field):
        slot = tally[0] % 2
        tally[0] += 1
        n = sizes[level]
        wide = ceil8(n)
        for dim in (1, 2, 0):
            last = counts[dim] - 1

            @pl.when(place[dim] < last)
            def _():
                face_copy(level, field, slot, dim, True).start()

            @pl.when(place[dim] > 0)
            def _():
                face_copy(level, field, slot, dim, False).start()
        for dim in (0, 2, 1):
            last = counts[dim] - 1

            @pl.when(place[dim] < last)
            def _():
                face_copy(level, field, slot, dim, True).wait_send()
                face_copy(level, field, slot, dim, False).wait_recv()

            @pl.when(place[dim] > 0)
            def _():
                face_copy(level, field, slot, dim, False).wait_send()
                face_copy(level, field, slot, dim, True).wait_recv()
        field[0, TOP : TOP + wide, :] = recv[slot, 0, 0:wide, :]
        field[n + 1, TOP : TOP + wide, :] = recv[slot, 1, 0:wide, :]
        _, _, f, _, diag, _, bx, by, bz, hz, _ = levels[level]
        lane = iota((n, LANES), 1)
        row = iota((n, LANES), 0)

        def remainder(i):
            here = field[i + 1, TOP : TOP + n, :]
            low_y = jnp.where(
                row == 0, recv[slot, 2, pl.ds(i, 1), :], field[i + 1, TOP - 1 : TOP - 1 + n, :]
            )
            high_y = jnp.where(
                row == n - 1, recv[slot, 3, pl.ds(i, 1), :], field[i + 1, TOP + 1 : TOP + 1 + n, :]
            )
            low_z = jnp.where(
                lane == 0, lane_roll(recv[slot, 4, 0:n, :], LANES - i), lane_roll(here, 1)
            )
            high_z = jnp.where(
                lane == n - 1,
                lane_roll(recv[slot, 5, 0:n, :], 2 * n - 2 - i),
                lane_roll(here, -1),
            )
            out = f[i, 0:n, :] - diag[i, 0:n, :] * here
            out = out + bx[i, 0:n, :] * field[i, TOP : TOP + n, :]
            out = out + bx[i + 1, 0:n, :] * field[i + 2, TOP : TOP + n, :]
            flow = by[i, 0:n, :] * low_y + by[i, 1 : n + 1, :] * high_y
            flow = flow + bz[i, 0:n, :] * low_z + hz[i, 0:n, :] * high_z
            return out + flow
        return remainder

    def chebyshev_sweep(level, old, new, factor):
        keep, gain = factor
        remainder = exchange(level, old)
        n = sizes[level]
        dd, inv = levels[level][3], levels[level][5]

        def make(i):
            step = gain * (inv[i, 0:n, :] * remainder(i))
            if keep:
                step = step + keep * dd[i, 0:n, :]
            dd[i, 0:n, :] = step
            return old[i + 1, TOP : TOP + n, :] + step
        sweep_planes(level, new, make)

    for level in range(deepest):
        n, nc = sizes[level], sizes[level + 1]
        xa, xb, f, dd, diag, inv = levels[level][:6]

        def begin(i):
            step = factors[0][1] * (inv[i, 0:n, :] * f[i, 0:n, :])
            dd[i, 0:n, :] = step
            return step
        sweep_planes(level, xa, begin)
        chebyshev_sweep(level, xa, xb, factors[1])
        chebyshev_sweep(level, xb, xa, factors[2])
        remainder = exchange(level, xa)

        def pick(i):
            xb[i + 1, TOP : TOP + n, :] = remainder(2 * i) + remainder(2 * i + 1)
            return (
                xb[i + 1, pl.ds(TOP, nc, stride=2), :] + xb[i + 1, pl.ds(TOP + 1, nc, stride=2), :]
            )
        transfer(nc, pick, pair_sum, 0.125, to(levels[level + 1][2]))

    m = sizes[deepest]
    f_b, bx_b, by_b, bz_b, cells_b = [levels[deepest][k] for k in (2, 6, 7, 8, 10)]
    gsend[...] = jnp.zeros_like(gsend)
    for which, ref in enumerate((f_b, bx_b, by_b, bz_b, cells_b)):
        for i in range(m):
            start = (which * m + i) * m
            gsend[start : start + m, :] = lane_roll(ref[i, 0:m, :], place[2] * m)

    def line(dim, src, dst, ssem, rsem):
        total = counts[dim]

        def copy(off):
            return pltpu.make_async_remote_copy(
                src_ref=src,
                dst_ref=dst.at[place[dim]],
                send_sem=ssem.at[dim, off],
                recv_sem=rsem.at[dim, off],
                device_id={AXES[dim]: lax.rem(place[dim] + off, total)},
                device_id_type=pl.DeviceIdType.MESH,
            )
        for off in range(1, total):
            copy(off).start()
        dst[place[dim]] = src[...]
        for off in range(1, total):
            copy(off).wait()

    line(2, gsend, gz_recv, gsend_sem, grecv_sem)
    merged = gz_recv[0]
    for k in range(1, counts[2]):
        merged = merged + gz_recv[k]
    gy_send[...] = merged
    line(1, gy_send, gy_recv, gsend_sem, grecv_sem)
    line(0, gy_recv, gx_recv, gsend_sem, grecv_sem)

    tall = glob.shape[2]
    mx, my, mz = m * counts[0], m * counts[1], m * counts[2]
    glob[...] = jnp.zeros_like(glob)
    for which in range(5):
        for a in range(counts[0]):
            for b in range(counts[1]):
                for i in range(m):
                    start = (which * m + i) * m
                    glob[which, a * m + i, b * m : (b + 1) * m, :] = gx_recv[
                        a, b, start : start + m, :
                    ]
    lane = iota((tall, LANES), 1)
    row = iota((tall, LANES), 0)
    zero = jnp.zeros((tall, LANES), jnp.float32)
    for i in range(mx):
        hy = jnp.where(row < my - 1, pltpu.roll(glob[2, i], tall - 1, 0), 0.0)
        hz = jnp.where(lane < mz - 1, pltpu.roll(glob[3, i], LANES - 1, 1), 0.0)
        hx = glob[1, i + 1] if i + 1 < mx else zero
        glob[5, i] = hy
        glob[6, i] = hz
        glob[7, i] = glob[4, i] + glob[1, i] + hx + glob[2, i] + hy + glob[3, i] + hz

    def total(parts):
        acc = parts[0]
        for part in parts[1:]:
            acc = acc + part
        return jnp.sum(jnp.sum(acc, axis=0, keepdims=True), axis=1, keepdims=True)

    rest = [glob[0, i] for i in range(mx)]
    search = rest
    iterate = [zero] * mx
    norm_now = total([v * v for v in rest])
    for step in range(BOTTOM):
        applied = []
        for i in range(mx):
            v = search[i]
            out = glob[7, i] * v
            if i:
                out = out - glob[1, i] * search[i - 1]
            if i + 1 < mx:
                out = out - glob[1, i + 1] * search[i + 1]
            out = out - glob[2, i] * pltpu.roll(v, 1, 0) - glob[5, i] * pltpu.roll(v, tall - 1, 0)
            out = out - glob[3, i] * pltpu.roll(v, 1, 1) - glob[6, i] * pltpu.roll(v, LANES - 1, 1)
            applied.append(out)
        size = norm_now / total([a * b for a, b in zip(search, applied)])
        iterate = [e + size * v for e, v in zip(iterate, search)]
        if step + 1 < BOTTOM:
            rest = [r - size * q for r, q in zip(rest, applied)]
            norm_next = total([v * v for v in rest])
            ratio = norm_next / norm_now
            search = [r + ratio * v for r, v in zip(rest, search)]
            norm_now = norm_next
    for i in range(mx):
        whole[i] = iterate[i]
    below = levels[deepest][3]
    lane = iota((m, LANES), 1)
    for i in range(m):
        plane = whole[place[0] * m + i]
        plane = pltpu.roll(plane, lax.rem(tall - place[1] * m + tall, tall), 0)
        plane = pltpu.roll(plane, lax.rem(LANES - place[2] * m + LANES, LANES), 1)
        below[i, 0:m, :] = jnp.where(lane < m, plane[0:m], 0.0)

    coarse = lambda i: below[i, 0:m, :]
    for level in reversed(range(deepest)):
        n, nc = sizes[level], sizes[level + 1]
        xa, xb = levels[level][:2]

        def add(start, chunk, rows, out):
            for k in range(chunk):
                for odd_x in range(2):
                    plane = 2 * (start + k) + odd_x + 1
                    for odd_y in range(2):
                        at_rows = pl.ds(TOP + odd_y, nc, stride=2)
                        xa[plane, at_rows, :] = xa[plane, at_rows, :] + out[k, 0:nc]
        transfer(nc, coarse, spread, 1.0, add)
        sweep_planes(level, xa, lambda i: xa[i + 1, TOP : TOP + n, :])
        chebyshev_sweep(level, xa, xb, factors[0])
        chebyshev_sweep(level, xb, xa, factors[1])
        chebyshev_sweep(level, xa, xb, factors[2])
        coarse = functools.partial(lambda ref, count, i: ref[i + 1, TOP : TOP + count, :], xb, n)

    n = sizes[0]
    xa, xb = levels[0][:2]
    remainder = exchange(0, xb)

    def finish(i, acc):
        out = remainder(i)
        sol_ref[i] = xb[i + 1, TOP : TOP + n, 0:n]
        res_ref[i] = out[:, 0:n]
        return acc + out * out
    res_square = loop(n, finish, jnp.zeros((n, LANES), jnp.float32))
    nsend[0, 0:1, :] = jnp.sum(res_square, axis=0, keepdims=True)
    nsend[0, 1:2, :] = jnp.sum(rhs_square, axis=0, keepdims=True)
    nsend[0, 2:8, :] = jnp.zeros((6, LANES), jnp.float32)
    for step, (dim, got) in enumerate(((2, nz_recv), (1, ny_recv), (0, nx_recv))):
        line(dim, nsend.at[step], got, nsend_sem, nrecv_sem)
        acc = got[0]
        for k in range(1, counts[dim]):
            acc = acc + got[k]
        if step < 2:
            nsend[step + 1] = acc
    sums = jnp.sum(acc, axis=1, keepdims=True)
    norm_ref[...] = jnp.broadcast_to(jnp.sqrt(sums[0:1] / sums[1:2]), norm_ref.shape)


def body(counts, right_side, face_coef, absorption):
    n = right_side.shape[0]
    sizes = [n >> level for level in range(LEVELS)]
    f32 = jnp.float32
    scratch = []
    for size in sizes:
        wide = ceil8(size)
        flat = pltpu.VMEM((size, wide, LANES), f32)
        field = pltpu.VMEM((size + 2, wide + 2 * TOP, LANES), f32)
        scratch += [field, field, flat, flat, flat, flat]
        scratch += [
            pltpu.VMEM((size + 1, wide, LANES), f32),
            pltpu.VMEM((size, wide + 8, LANES), f32),
            flat, flat, flat,
        ]
    wide = ceil8(n)
    half = ceil8(n // 2)
    m = sizes[-1]
    packed = ceil8(5 * m * m)
    tall = (m * counts[1] + 8) // 8 * 8
    most = max(counts)
    scratch += [
        pltpu.VMEM((n // 2, half, LANES), f32),
        pltpu.VMEM((2, wide, LANES), f32),
        pltpu.VMEM((2, wide, LANES), f32),
        pltpu.VMEM((2, 6, wide, LANES), f32),
        pltpu.VMEM((LEVELS - 1, wide, LANES), f32),
        pltpu.VMEM((LEVELS - 1, wide, LANES), f32),
        pltpu.VMEM((LEVELS - 1, 3, wide, LANES), f32),
        pltpu.VMEM((packed, LANES), f32),
        pltpu.VMEM((counts[2], packed, LANES), f32),
        pltpu.VMEM((packed, LANES), f32),
        pltpu.VMEM((counts[1], packed, LANES), f32),
        pltpu.VMEM((counts[0], counts[1], packed, LANES), f32),
        pltpu.VMEM((8, m * counts[0], tall, LANES), f32),
        pltpu.VMEM((m * counts[0], tall, LANES), f32),
        pltpu.VMEM((3, 8, LANES), f32),
        pltpu.VMEM((counts[2], 8, LANES), f32),
        pltpu.VMEM((counts[1], 8, LANES), f32),
        pltpu.VMEM((counts[0], 8, LANES), f32),
        pltpu.SemaphoreType.DMA((2, 6)),
        pltpu.SemaphoreType.DMA((2, 6)),
        pltpu.SemaphoreType.DMA((LEVELS - 1, 3)),
        pltpu.SemaphoreType.DMA((LEVELS - 1, 3)),
        pltpu.SemaphoreType.DMA((3, most)),
        pltpu.SemaphoreType.DMA((3, most)),
        pltpu.SemaphoreType.DMA((3, most)),
        pltpu.SemaphoreType.DMA((3, most)),
    ]
    vmem = pl.BlockSpec(memory_space=pltpu.VMEM)
    answer, residual, norm = pl.pallas_call(
        functools.partial(kernel, sizes, counts),
        out_shape=(
            jax.ShapeDtypeStruct(right_side.shape, f32),
            jax.ShapeDtypeStruct(right_side.shape, f32),
            jax.ShapeDtypeStruct((8, LANES), f32),
        ),
        in_specs=[vmem] * 3,
        out_specs=(vmem,) * 3,
        scratch_shapes=scratch,
        compiler_params=pltpu.CompilerParams(
            has_side_effects=True, vmem_limit_bytes=60 * 1024 * 1024
        ),
        name="vcycle",
    )(right_side, face_coef, absorption)
    return answer, residual, norm[0, 0]


def solution(mesh):
    counts = tuple(mesh.shape[a] for a in AXES)
    return jax.shard_map(
        functools.partial(body, counts),
        mesh=mesh,
        in_specs=(P("gx", "gy", "gz"), P(None, "gx", "gy", "gz"), P("gx", "gy", "gz")),
        out_specs=(P("gx", "gy", "gz"), P("gx", "gy", "gz"), P()),
        check_vma=False,
    )
```
